256 devices in a mesh: groups: 2 (over y), seq: 2 (over core), row: 16 (over z), col: 4 (over x).
Axes of the slice: x: 4, y: 2, z: 16, core: 2. Of those that a mesh axis runs over, the one named last changes fastest.
The devices are a block of a 4x16x16 slice.
Arguments:
- paired_left: bfloat16 [1024, 32, 512], P(('groups', 'seq', 'col'), None, 'row'), parts along dimension 0, may hold values from -24 to 24
- paired_right: bfloat16 [1024, 32, 512], P(('groups', 'seq', 'row'), None, 'col'), parts along dimension 0, may hold values from -24 to 24
- unpaired_left: bfloat16 [2048, 32, 512], P(('groups', 'seq', 'col'), None, 'row'), parts along dimension 0, may hold values from -24 to 24
- unpaired_right: bfloat16 [2048, 32, 512], P(('groups', 'seq', 'row'), None, 'col'), parts along dimension 0, may hold values from -24 to 24
- out_weight: bfloat16 [1024, 128], replicated, may hold values from -0.1875 to 0.1875
- out_bias: float32 [128], replicated, may hold values from -6 to 6
- chain_lengths: int32 [24], P('groups'), parts along dimension 0, may hold values from 1 to 128, 512 in all
- unpaired_depths: int32 [24], P('groups'), parts along dimension 0, may hold values from 256 to 1024
Outputs:
- pair_update: bfloat16 [1024, 512, 128], P(('groups', 'row'), ('col', 'seq')), parts along dimension 0
The draws below stay inside these ranges and needn't reach their ends.
There are 2 independent parts, one for each index of `groups`. The reference program is written for one: setup_inputs(seed, part) draws one part's arguments, and reference() takes and returns one part's arrays. A program takes and returns all parts, laid end to end along the dimension named above; an argument that names none is the same for every part. Nothing has to cross between parts.
Inputs may be any that keep to these rules, and one draw needn't show every extreme that they name: `chain_lengths`: chain lengths sum to 512. `unpaired_depths`: rows of the unpaired MSA at or beyond a chain's depth are padding.
All inputs are finite; a program needn't handle non-finite values.
Results may differ from the reference program's by a relative error of at most 0.0034.
Values may be sent and summed in bfloat16 or wider, within the bound.
A program may use at most 64 MiB of HBM per device.

```python
import math
import jax
import jax.numpy as jnp
import numpy as np
from jax import lax

C = 32
Z = 128
CHAINS = 12
S_P = 512
DMAX = 1024
N = 512
N_SEQ = 2


def place_ends(result, own_key, least, top_value):
    longest = result.shape.index(max(result.shape))
    spots = []
    for shift in (0, 1):
        where = [jax.random.randint(jax.random.fold_in(own_key, axis), (), 0, length) for axis, length in enumerate(result.shape)]
        where[longest] = (where[longest] + shift) % result.shape[longest]
        spots.append(tuple(where))
    return result.at[spots[0]].set(least).at[spots[1]].set(top_value)


def block_scale(key, shape, shards, least, high):
    level = 1.0
    for axis_at, parts in shards:
        steps = jax.random.uniform(jax.random.fold_in(jax.random.fold_in(key, 6), axis_at), (parts,), jnp.float32, least / len(shards), high / len(shards))
        level = level * jnp.repeat(jnp.exp(steps), shape[axis_at] // parts).reshape((-1,) + (1,) * (len(shape) - 1 - axis_at))
    return level


def length_profile(number_of, total, bound, skew):
    weights = [(1 << 20) // math.isqrt(rank ** skew) + 1 for rank in range(2, number_of + 1)]
    spare, given = total - bound - (number_of - 1), [1] * (number_of - 1)
    while spare > 0:
        free = [i for i in range(number_of - 1) if given[i] < bound]
        pool, left = sum([weights[i] for i in free]), spare
        for i in free:
            more = min(bound - given[i], max(1, left * weights[i] // pool), spare)
            given[i] = given[i] + more
            spare = spare - more
    return np.array([bound] + given)


def ragged_sizes(key, number_of, total, most, lean):
    if number_of == 2:
        one = jax.random.randint(key, (), max(1, total - most), min(most, total - 1) + 1)
        return jnp.stack([one, total - one])
    sizes = jnp.asarray(length_profile(number_of, total, most, lean), jnp.int32)
    couples = (number_of - 1) // 2
    source_of, taker = sizes[1:1 + 2 * couples:2], sizes[2:2 + 2 * couples:2]
    slack = jnp.minimum(source_of - 1, most - taker)
    moved = jax.random.randint(jax.random.fold_in(key, 1), (couples,), 0, 1 << 20) % (slack + 1)
    sizes = sizes.at[1:1 + 2 * couples:2].set(source_of - moved).at[2:2 + 2 * couples:2].set(taker + moved)
    return sizes[jax.random.permutation(jax.random.fold_in(key, 2), number_of)]


def scatter_about(own_key, shape, spread, bound, split=(), kind=jnp.bfloat16):
    factor_of = block_scale(own_key, shape, split, -0.22, 0.18) if split else 1.0
    values = jax.random.normal(own_key, shape, jnp.float32) * spread * factor_of
    return jnp.minimum(jnp.maximum(values, -bound), bound).astype(kind)


def setup_inputs(seed: int = 0, part: int = 0) -> dict:
    streams_of = jax.random.split(jax.random.key(seed), 9)
    part_keys = jax.random.split(jax.random.fold_in(streams_of[8], part), 9)
    paired_left = scatter_about(part_keys[0], (S_P, C, N), 4.0, 24.0, ((0, 8), (2, 16)))
    paired_right = scatter_about(part_keys[1], (S_P, C, N), 4.0, 24.0, ((0, 32), (2, 4)))
    unpaired_left = scatter_about(part_keys[2], (DMAX, C, N), 4.0, 24.0, ((0, 8), (2, 16)))
    unpaired_right = scatter_about(part_keys[3], (DMAX, C, N), 4.0, 24.0, ((0, 32), (2, 4)))
    out_weight = scatter_about(streams_of[4], (C * C, Z), (C * C) ** -0.5, 0.1875)
    out_bias = scatter_about(streams_of[5], (Z,), 1.0, 6.0, (), jnp.float32)
    chain_lengths = ragged_sizes(part_keys[6], CHAINS, N, N // 4, 1).astype(jnp.int32)
    unpaired_depths = place_ends(jax.random.randint(part_keys[7], (CHAINS,), DMAX // 4, DMAX + 1), jax.random.fold_in(part_keys[7], 1), DMAX // 4, DMAX).astype(jnp.int32)
    return {"paired_left": paired_left, "paired_right": paired_right, "unpaired_left": unpaired_left, "unpaired_right": unpaired_right, "out_weight": out_weight, "out_bias": out_bias, "chain_lengths": chain_lengths, "unpaired_depths": unpaired_depths}


def chain_tables(chain_lengths, unpaired_depths):
    positions = jnp.arange(N, dtype=jnp.int32)
    chain_ends = jnp.cumsum(chain_lengths).astype(jnp.int32)
    chain_of = jnp.sum((positions[:, None] >= chain_ends[None, :]).astype(jnp.int32), axis=1).astype(jnp.int32)
    onehot = chain_of[:, None] == jnp.arange(CHAINS, dtype=jnp.int32)[None, :]
    depth_of = jnp.sum(jnp.where(onehot, unpaired_depths[None, :], 0), axis=1).astype(jnp.int32)
    return chain_of, depth_of


def reference(paired_left, paired_right, unpaired_left, unpaired_right, out_weight, out_bias, chain_lengths, unpaired_depths):
    chain_of, depth_of = chain_tables(chain_lengths, unpaired_depths)
    free_ids = jnp.arange(DMAX, dtype=jnp.int32)
    live = (free_ids[:, None] < depth_of[None, :]).astype(unpaired_left.dtype)
    masked_left = unpaired_left * live[:, None, :]
    paired_group = S_P // N_SEQ
    free_group = DMAX // N_SEQ
    ref_rows = 8

    def one_block(block_index):
        offset = (block_index * ref_rows).astype(jnp.int32)
        chain_block = lax.dynamic_slice_in_dim(chain_of, offset, ref_rows, 0)
        depth_block = lax.dynamic_slice_in_dim(depth_of, offset, ref_rows, 0)
        same_chain = (chain_block[:, None] == chain_of[None, :]).astype(jnp.float32)
        summed = jnp.zeros((ref_rows, N, Z), jnp.float32)
        for group in range(N_SEQ):
            left_pair = lax.dynamic_slice_in_dim(paired_left[group * paired_group:(group + 1) * paired_group], offset, ref_rows, 2).astype(jnp.float32)
            right_pair = paired_right[group * paired_group:(group + 1) * paired_group].astype(jnp.float32)
            left_free = lax.dynamic_slice_in_dim(masked_left[group * free_group:(group + 1) * free_group], offset, ref_rows, 2).astype(jnp.float32)
            right_free = unpaired_right[group * free_group:(group + 1) * free_group].astype(jnp.float32)
            outer = jnp.einsum('sci,sdj->ijcd', left_pair, right_pair)
            outer = outer + jnp.einsum('sci,sdj->ijcd', left_free, right_free) * same_chain[:, :, None, None]
            outer_product = outer.astype(jnp.bfloat16).reshape(ref_rows * N, C * C)
            summed = summed + jnp.dot(outer_product, out_weight, preferred_element_type=jnp.float32).reshape(ref_rows, N, Z)
        denominator = S_P + same_chain * depth_block[:, None].astype(jnp.float32)
        return (summed / denominator[:, :, None] + out_bias).astype(jnp.bfloat16)

    blocks = lax.map(one_block, jnp.arange(N // ref_rows, dtype=jnp.int32))
    return blocks.reshape(N, N, Z)
```

```python
import functools

import jax
import jax.numpy as jnp
from jax import lax
from jax.experimental import pallas as pl
from jax.experimental.pallas import tpu as pltpu
from jax.sharding import PartitionSpec as P

MESH = pl.DeviceIdType.MESH
F32 = jnp.float32
BF16 = jnp.bfloat16
PHASES = 4
ROWS_PER_UNIT = 4


def kernel(
    dims,
    rp_ref,
    ru_ref,
    lp_ref,
    lu_ref,
    wt_ref,
    bias_ref,
    len_ref,
    dep_ref,
    out_ref,
    rbp,
    rbu,
    lbp,
    lbu,
    ltp,
    ltu,
    acc,
    part,
    got,
    same_ref,
    scale_ref,
    send_r,
    recv_r,
    send_l,
    recv_l,
    send_x,
    recv_x,
):
    nrow, ncol, nseq, chans, chains, ni, nj, nz, s_paired = dims
    me = lax.axis_index("row")
    col = lax.axis_index("col")
    seq = lax.axis_index("seq")
    right, left = lax.rem(me + 1, nrow), lax.rem(me + nrow - 1, nrow)
    other = 1 - seq
    lanes = chans * nj // PHASES
    per_phase = chans // PHASES

    barrier = pltpu.get_barrier_semaphore()
    for nb in (right, left):
        pl.semaphore_signal(barrier, inc=1, device_id={"row": nb}, device_id_type=MESH)
    for k in range(1, ncol):
        pl.semaphore_signal(
            barrier, inc=1, device_id={"col": lax.rem(col + k, ncol)}, device_id_type=MESH
        )
    pl.semaphore_signal(barrier, inc=1, device_id={"seq": other}, device_id_type=MESH)
    pl.semaphore_wait(barrier, 2 + ncol - 1 + 1)

    half = nrow // 2

    def steps(way, ph):
        return half if (ph + way) % 2 == 0 else half - 1

    def block(way, t):
        return lax.rem(me - t + nrow, nrow) if way == 0 else lax.rem(me + t, nrow)

    def ring(way, ph, t, kind):
        q = block(way, t - 1)
        buf, own = ((rbp, rp_ref), (rbu, ru_ref))[kind]
        part_of = pl.ds(ph * lanes, lanes)
        src = own.at[:, part_of] if t == 1 else buf.at[q, :, part_of]
        at = ((way * PHASES + ph) * half + t - 1) * 2 + kind
        return pltpu.make_async_remote_copy(
            src_ref=src,
            dst_ref=buf.at[q, :, part_of],
            send_sem=send_r.at[at],
            recv_sem=recv_r.at[at],
            device_id={"row": right if way == 0 else left},
            device_id_type=MESH,
        )

    def arrival(way, ph, t, kind):
        q = block(way, t)
        buf = (rbp, rbu)[kind]
        part_of = pl.ds(ph * lanes, lanes)
        at = ((way * PHASES + ph) * half + t - 1) * 2 + kind
        return pltpu.make_async_remote_copy(
            src_ref=buf.at[q, :, part_of],
            dst_ref=buf.at[q, :, part_of],
            send_sem=send_r.at[at],
            recv_sem=recv_r.at[at],
            device_id={"row": right if way == 0 else left},
            device_id_type=MESH,
        )

    def first_sends(phases):
        for kind in (1, 0):
            for ph in phases:
                for way in (0, 1):
                    ring(way, ph, 1, kind).start()

    def left_copy(k, kind, incoming):
        own, buf = ((lp_ref, lbp), (lu_ref, lbu))[kind]
        at = (k - 1) * 2 + kind
        slot = lax.rem(col - k + ncol, ncol) if incoming else col
        return pltpu.make_async_remote_copy(
            src_ref=own,
            dst_ref=buf.at[slot],
            send_sem=send_l.at[at],
            recv_sem=recv_l.at[at],
            device_id={"col": lax.rem(col + k, ncol)},
            device_id_type=MESH,
        )

    first_sends((0, 1))
    for k in range(1, ncol):
        for kind in (0, 1):
            left_copy(k, kind, False).start()

    rbp[pl.ds(me, 1)] = rp_ref[...][None]
    rbu[pl.ds(me, 1)] = ru_ref[...][None]
    lbp[pl.ds(col, 1)] = lp_ref[...][None]
    lbu[pl.ds(col, 1)] = lu_ref[...][None]
    acc[...] = jnp.zeros_like(acc)

    pos_i = lax.broadcasted_iota(jnp.int32, (ni, nj), 0) + me * ni
    pos_j = lax.broadcasted_iota(jnp.int32, (ni, nj), 1) + col * nj
    chain_i = jnp.zeros((ni, nj), jnp.int32)
    chain_j = jnp.zeros((ni, nj), jnp.int32)
    end = jnp.int32(0)
    ends = []
    for k in range(chains):
        end = end + len_ref[k]
        ends.append(end)
        chain_i = chain_i + (pos_i >= end).astype(jnp.int32)
        chain_j = chain_j + (pos_j >= end).astype(jnp.int32)
    same = (chain_i == chain_j).astype(F32)
    depth_i = jnp.zeros((ni, nj), F32)
    for k in range(chains):
        depth_i = depth_i + jnp.where(chain_i == k, dep_ref[k].astype(F32), 0.0)
    same_ref[...] = same
    scale_ref[...] = 1.0 / (s_paired + same * depth_i)

    def forward(ph, t):
        for kind in (1, 0):
            for way in (0, 1):
                if t <= steps(way, ph):
                    arrival(way, ph, t, kind).wait_recv()
                    if t < steps(way, ph):
                        ring(way, ph, t + 1, kind).start()

    free_rows = lbu.shape[0] * lbu.shape[1]
    block_rows = 128

    def left_ready():
        for k in range(1, ncol):
            for kind in (0, 1):
                left_copy(k, kind, True).wait_recv()
        ltp[...] = lbp[...].reshape(-1, ni * chans).T
        ltu[...] = lbu[...].reshape(-1, ni * chans).T

        def mask_rows(b, _):
            rows = pl.ds(pl.multiple_of(b * block_rows, block_rows), block_rows)
            shape = (block_rows, free_rows)
            pos = (lax.broadcasted_iota(jnp.int32, shape, 0) + b * block_rows) // chans + me * ni
            ids = lax.broadcasted_iota(jnp.int32, shape, 1) + seq * free_rows
            depth = jnp.zeros(shape, jnp.int32)
            for k in range(chains):
                low = ends[k - 1] if k else 0
                depth = jnp.where((pos >= low) & (pos < ends[k]), dep_ref[k], depth)
            live = jnp.where(ids < depth, 1.0, 0.0).astype(BF16)
            ltu[rows, :] = ltu[rows, :] * live
            return 0

        lax.fori_loop(0, ni * chans // block_rows, mask_rows, 0)

    def unit(ph, ib):
        rows = ROWS_PER_UNIT * chans
        at = pl.ds(pl.multiple_of(ib * rows, rows), rows)
        part_of = pl.ds(ph * lanes, lanes)
        kp = rbp.shape[0] * rbp.shape[1]
        ku = rbu.shape[0] * rbu.shape[1]
        a = jnp.dot(ltp[at, :], rbp[:, :, part_of].reshape(kp, lanes), preferred_element_type=F32)
        b = jnp.dot(ltu[at, :], rbu[:, :, part_of].reshape(ku, lanes), preferred_element_type=F32)
        w = wt_ref[:, ph * per_phase * chans : (ph + 1) * per_phase * chans]
        for pair in range(ROWS_PER_UNIT // 2):
            cols = []
            for ii in (2 * pair, 2 * pair + 1):
                m = same_ref[pl.ds(ib * ROWS_PER_UNIT + ii, 1), :]
                tiles = []
                for d in range(per_phase):
                    rs = slice(ii * chans, (ii + 1) * chans)
                    ls = slice(d * nj, (d + 1) * nj)
                    tiles.append((a[rs, ls] + b[rs, ls] * m).astype(BF16))
                cols.append(jnp.concatenate(tiles, axis=0))
            x = jnp.concatenate(cols, axis=1)
            to = pl.ds(pl.multiple_of((ib * ROWS_PER_UNIT + 2 * pair) * nj, 2 * nj), 2 * nj)
            acc[:, to] += jnp.dot(w, x, preferred_element_type=F32)

    units = ni // ROWS_PER_UNIT
    for t in range(1, half + 1):
        for ph in (0, 1):
            forward(ph, t)
            if t == half:
                pass
        if t == half - 1:
            first_sends((2, 3))
        if t == half // 2:
            left_ready()
    for t in range(1, half + 1):
        for ph in (2, 3):
            forward(ph, t)

        def two(n, _, t=t):
            unit(0, n + (t - 1))
            unit(1, n + (t - 1))
            return 0

        lax.fori_loop(0, 1, two, 0)

    def tail(n, _):
        unit(2, n)
        unit(3, n)
        return 0

    lax.fori_loop(0, units, tail, 0)

    def turn(i, _):
        tile = acc[:, pl.ds(pl.multiple_of(i * nj, nj), nj)] * scale_ref[pl.ds(i, 1), :]
        part[pl.ds(i, 1)] = tile.T[None]
        return 0

    lax.fori_loop(0, ni, turn, 0)
    hj = nj // nseq
    swap = pltpu.make_async_remote_copy(
        src_ref=part.at[:, pl.ds(pl.multiple_of(other * hj, hj), hj), :],
        dst_ref=got,
        send_sem=send_x,
        recv_sem=recv_x,
        device_id={"seq": other},
        device_id_type=MESH,
    )
    swap.start()
    swap.wait_recv()

    def finish(i, _):
        mine = part[pl.ds(i, 1), pl.ds(pl.multiple_of(seq * hj, hj), hj), :]
        out_ref[pl.ds(i, 1)] = (mine + got[pl.ds(i, 1)] + bias_ref[...][None]).astype(BF16)
        return 0

    lax.fori_loop(0, ni, finish, 0)

    swap.wait_send()
    for k in range(1, ncol):
        for kind in (0, 1):
            left_copy(k, kind, False).wait_send()
    for ph in range(PHASES):
        for way in (0, 1):
            for t in range(1, steps(way, ph) + 1):
                for kind in (0, 1):
                    ring(way, ph, t, kind).wait_send()


def body(sizes, pl_, pr, ul, ur, weight, bias, lengths, depths):
    nrow, ncol, nseq = sizes
    chans, ni = pl_.shape[1], pl_.shape[2]
    nj = pr.shape[2]
    nz = weight.shape[1]
    rp = pr.reshape(pr.shape[0], chans * nj)
    ru = ur.reshape(ur.shape[0], chans * nj)
    lp = jnp.transpose(pl_, (0, 2, 1)).reshape(pl_.shape[0], ni * chans)
    lu = jnp.transpose(ul, (0, 2, 1)).reshape(ul.shape[0], ni * chans)
    wt = jnp.transpose(weight.reshape(chans, chans, nz), (2, 1, 0)).reshape(nz, chans * chans)
    s_paired = float(pr.shape[0] * nrow * nseq)
    dims = (nrow, ncol, nseq, chans, lengths.shape[0], ni, nj, nz, s_paired)
    half = nrow // 2
    vm = pl.BlockSpec(memory_space=pltpu.VMEM)
    sm = pl.BlockSpec(memory_space=pltpu.SMEM)
    dma = pltpu.SemaphoreType.DMA
    hj = nj // nseq
    return pl.pallas_call(
        functools.partial(kernel, dims),
        out_shape=jax.ShapeDtypeStruct((ni, hj, nz), BF16),
        in_specs=[vm] * 6 + [sm] * 2,
        out_specs=vm,
        scratch_shapes=[
            pltpu.VMEM((nrow, pr.shape[0], chans * nj), BF16),
            pltpu.VMEM((nrow, ur.shape[0], chans * nj), BF16),
            pltpu.VMEM((ncol, *lp.shape), BF16),
            pltpu.VMEM((ncol, *lu.shape), BF16),
            pltpu.VMEM((ni * chans, ncol * lp.shape[0]), BF16),
            pltpu.VMEM((ni * chans, ncol * lu.shape[0]), BF16),
            pltpu.VMEM((nz, ni * nj), F32),
            pltpu.VMEM((ni, nj, nz), F32),
            pltpu.VMEM((ni, hj, nz), F32),
            pltpu.VMEM((ni, nj), F32),
            pltpu.VMEM((ni, nj), F32),
            dma((2 * PHASES * half * 2,)),
            dma((2 * PHASES * half * 2,)),
            dma(((ncol - 1) * 2,)),
            dma(((ncol - 1) * 2,)),
            dma,
            dma,
        ],
        compiler_params=pltpu.CompilerParams(
            collective_id=0, has_side_effects=True, vmem_limit_bytes=48 * 1024 * 1024
        ),
    )(rp, ru, lp, lu, wt, bias.reshape(1, nz), lengths, depths)


def solution(mesh):
    sizes = (mesh.shape["row"], mesh.shape["col"], mesh.shape["seq"])
    return jax.shard_map(
        functools.partial(body, sizes),
        mesh=mesh,
        in_specs=(
            P(("groups", "seq", "col"), None, "row"),
            P(("groups", "seq", "row"), None, "col"),
            P(("groups", "seq", "col"), None, "row"),
            P(("groups", "seq", "row"), None, "col"),
            P(),
            P(),
            P("groups"),
            P("groups"),
        ),
        out_specs=P(("groups", "row"), ("col", "seq"), None),
        check_vma=False,
    )
```

```python
import functools

import jax
import jax.numpy as jnp
from jax import lax
from jax.experimental import pallas as pl
from jax.experimental.pallas import tpu as pltpu
from jax.sharding import PartitionSpec as P

MESH = pl.DeviceIdType.MESH
F32 = jnp.float32
BF16 = jnp.bfloat16
PHASES = 4
ROWS_PER_UNIT = 4
STAGGER = 2


def kernel(
    dims,
    pr_ref,
    ur_ref,
    pl_ref,
    ul_ref,
    w_ref,
    bias_ref,
    len_ref,
    dep_ref,
    out_ref,
    prv,
    urv,
    plv,
    ulv,
    wv,
    perm,
    wt_ref,
    rbp,
    rbu,
    lbp,
    ltp,
    ltu,
    acc,
    part,
    got,
    same_ref,
    scale_ref,
    send_r,
    recv_r,
    send_l,
    recv_l,
    send_x,
    recv_x,
    load_sem,
):
    nrow, ncol, nseq, chans, chains, ni, nj, nz, s_paired = dims
    me = lax.axis_index("row")
    col = lax.axis_index("col")
    seq = lax.axis_index("seq")
    right, left = lax.rem(me + 1, nrow), lax.rem(me + nrow - 1, nrow)
    other = 1 - seq
    lanes = chans * nj // PHASES
    per_phase = chans // PHASES

    loads = [
        pltpu.make_async_copy(src, dst, load_sem.at[k])
        for k, (src, dst) in enumerate(
            ((pr_ref, prv), (ur_ref, urv), (pl_ref, plv), (ul_ref, ulv), (w_ref, wv))
        )
    ]
    for load in loads:
        load.start()

    barrier = pltpu.get_barrier_semaphore()
    for nb in (right, left):
        pl.semaphore_signal(barrier, inc=1, device_id={"row": nb}, device_id_type=MESH)
    for k in range(1, ncol):
        pl.semaphore_signal(
            barrier, inc=1, device_id={"col": lax.rem(col + k, ncol)}, device_id_type=MESH
        )
    pl.semaphore_signal(barrier, inc=1, device_id={"seq": other}, device_id_type=MESH)
    loads[0].wait()
    rbp[pl.ds(me, 1)] = prv[...].reshape(1, -1, chans * nj)
    loads[1].wait()
    rbu[pl.ds(me, 1)] = urv[...].reshape(1, -1, chans * nj)
    pl.semaphore_wait(barrier, 2 + ncol - 1 + 1)

    half = nrow // 2

    def steps(way, ph):
        return half if (ph + way) % 2 == 0 else half - 1

    def block(way, t):
        return lax.rem(me - t + nrow, nrow) if way == 0 else lax.rem(me + t, nrow)

    def ring(way, ph, t, kind):
        q = block(way, t - 1)
        buf = (rbp, rbu)[kind]
        part_of = pl.ds(ph * lanes, lanes)
        at = ((way * PHASES + ph) * half + t - 1) * 2 + kind
        return pltpu.make_async_remote_copy(
            src_ref=buf.at[q, :, part_of],
            dst_ref=buf.at[q, :, part_of],
            send_sem=send_r.at[at],
            recv_sem=recv_r.at[at],
            device_id={"row": right if way == 0 else left},
            device_id_type=MESH,
        )

    def arrival(way, ph, t, kind):
        q = block(way, t)
        buf = (rbp, rbu)[kind]
        part_of = pl.ds(ph * lanes, lanes)
        at = ((way * PHASES + ph) * half + t - 1) * 2 + kind
        return pltpu.make_async_remote_copy(
            src_ref=buf.at[q, :, part_of],
            dst_ref=buf.at[q, :, part_of],
            send_sem=send_r.at[at],
            recv_sem=recv_r.at[at],
            device_id={"row": right if way == 0 else left},
            device_id_type=MESH,
        )

    def first_sends(ph):
        for kind in (1, 0):
            for way in (0, 1):
                ring(way, ph, 1, kind).start()

    tall = ni * chans
    lu_rows = ulv.shape[2]

    def left_copy(k, kind, incoming):
        at = (k - 1) * 2 + kind
        slot = lax.rem(col - k + ncol, ncol) if incoming else col
        if kind == 0:
            src = dst = lbp.at[slot]
        else:
            src = dst = ltu.at[:, pl.ds(pl.multiple_of(slot * lu_rows, lu_rows), lu_rows)]
        return pltpu.make_async_remote_copy(
            src_ref=src,
            dst_ref=dst,
            send_sem=send_l.at[at],
            recv_sem=recv_l.at[at],
            device_id={"col": lax.rem(col + k, ncol)},
            device_id_type=MESH,
        )

    first_sends(0)

    block_rows = 128

    def fill(b, _):
        rows = pl.ds(pl.multiple_of(b * block_rows, block_rows), block_rows)
        r = lax.broadcasted_iota(jnp.int32, (block_rows, tall), 0) + b * block_rows
        k = lax.broadcasted_iota(jnp.int32, (block_rows, tall), 1)
        hit = k == (r % chans) * chans + r // chans
        perm[rows, :] = jnp.where(hit, 1.0, 0.0).astype(BF16)
        return 0

    lax.fori_loop(0, tall // block_rows, fill, 0)
    for load in loads[2:]:
        load.wait()
    lbp[pl.ds(col, 1)] = lax.dot_general(
        plv[...].reshape(tall, -1), perm[...], (((0,), (1,)), ((), ())),
        preferred_element_type=F32,
    ).astype(BF16)[None]
    ltu[:, pl.ds(pl.multiple_of(col * lu_rows, lu_rows), lu_rows)] = jnp.dot(
        perm[...], ulv[...].reshape(tall, -1), preferred_element_type=F32
    ).astype(BF16)
    for k in range(1, ncol):
        for kind in (0, 1):
            left_copy(k, kind, False).start()
    wt_ref[...] = jnp.dot(perm[...], wv[...], preferred_element_type=F32).T.astype(BF16)
    acc[...] = jnp.zeros_like(acc)

    pos_i = lax.broadcasted_iota(jnp.int32, (ni, nj), 0) + me * ni
    pos_j = lax.broadcasted_iota(jnp.int32, (ni, nj), 1) + col * nj
    chain_i = jnp.zeros((ni, nj), jnp.int32)
    chain_j = jnp.zeros((ni, nj), jnp.int32)
    end = jnp.int32(0)
    ends = []
    for k in range(chains):
        end = end + len_ref[k]
        ends.append(end)
        chain_i = chain_i + (pos_i >= end).astype(jnp.int32)
        chain_j = chain_j + (pos_j >= end).astype(jnp.int32)
    same = (chain_i == chain_j).astype(F32)
    depth_i = jnp.zeros((ni, nj), F32)
    for k in range(chains):
        depth_i = depth_i + jnp.where(chain_i == k, dep_ref[k].astype(F32), 0.0)
    same_ref[...] = same
    scale_ref[...] = 1.0 / (s_paired + same * depth_i)

    def forward(ph, t):
        for kind in (1, 0):
            for way in (0, 1):
                if t <= steps(way, ph):
                    arrival(way, ph, t, kind).wait_recv()
                    if t < steps(way, ph):
                        ring(way, ph, t + 1, kind).start()

    free_rows = ltu.shape[1]

    def left_ready():
        for k in range(1, ncol):
            for kind in (0, 1):
                left_copy(k, kind, True).wait_recv()
        for k in range(1, ncol):
            for kind in (0, 1):
                left_copy(k, kind, False).wait_send()
        ltp[...] = lbp[...].reshape(-1, tall).T

        def mask_rows(b, _):
            rows = pl.ds(pl.multiple_of(b * block_rows, block_rows), block_rows)
            shape = (block_rows, free_rows)
            pos = (lax.broadcasted_iota(jnp.int32, shape, 0) + b * block_rows) // chans + me * ni
            ids = lax.broadcasted_iota(jnp.int32, shape, 1) + seq * free_rows
            depth = jnp.zeros(shape, jnp.int32)
            for k in range(chains):
                low = ends[k - 1] if k else 0
                depth = jnp.where((pos >= low) & (pos < ends[k]), dep_ref[k], depth)
            live = jnp.where(ids < depth, 1.0, 0.0).astype(BF16)
            ltu[rows, :] = ltu[rows, :] * live
            return 0

        lax.fori_loop(0, ni * chans // block_rows, mask_rows, 0)

    def unit(ph, ib):
        rows = ROWS_PER_UNIT * chans
        at = pl.ds(pl.multiple_of(ib * rows, rows), rows)
        part_of = pl.ds(ph * lanes, lanes)
        kp = rbp.shape[0] * rbp.shape[1]
        ku = rbu.shape[0] * rbu.shape[1]
        a = jnp.dot(ltp[at, :], rbp[:, :, part_of].reshape(kp, lanes), preferred_element_type=F32)
        b = jnp.dot(ltu[at, :], rbu[:, :, part_of].reshape(ku, lanes), preferred_element_type=F32)
        w = wt_ref[:, ph * per_phase * chans : (ph + 1) * per_phase * chans]
        for pair in range(ROWS_PER_UNIT // 2):
            cols = []
            for ii in (2 * pair, 2 * pair + 1):
                m = same_ref[pl.ds(ib * ROWS_PER_UNIT + ii, 1), :]
                tiles = []
                for d in range(per_phase):
                    rs = slice(ii * chans, (ii + 1) * chans)
                    ls = slice(d * nj, (d + 1) * nj)
                    tiles.append((a[rs, ls] + b[rs, ls] * m).astype(BF16))
                cols.append(jnp.concatenate(tiles, axis=0))
            x = jnp.concatenate(cols, axis=1)
            to = pl.ds(pl.multiple_of((ib * ROWS_PER_UNIT + 2 * pair) * nj, 2 * nj), 2 * nj)
            acc[:, to] += jnp.dot(w, x, preferred_element_type=F32)

    units = ni // ROWS_PER_UNIT

    def work(ph, lo, hi):
        def one(n, _):
            unit(ph, n)
            return 0

        lax.fori_loop(lo, hi, one, 0)

    plan = {
        9: ((0, 0, 4),),
        10: ((0, 4, 8),),
        11: ((1, 0, 6),),
        12: ((1, 6, 8), (2, 0, 3)),
        13: ((2, 3, 8),),
    }
    for slot in range(1, half + STAGGER * (PHASES - 1) + 1):
        for ph in range(PHASES):
            t = slot - STAGGER * ph
            if 1 <= t <= half:
                forward(ph, t)
            if t == 0:
                first_sends(ph)
        if slot == half // 2 + 1:
            left_ready()
        for ph, lo, hi in plan.get(slot, ()):
            work(ph, lo, hi)

    hj = nj // nseq
    rows_of = ROWS_PER_UNIT

    def swap(n):
        at = pl.ds(n * rows_of, rows_of)
        return pltpu.make_async_remote_copy(
            src_ref=part.at[at, pl.ds(pl.multiple_of(other * hj, hj), hj), :],
            dst_ref=got.at[at],
            send_sem=send_x.at[n],
            recv_sem=recv_x.at[n],
            device_id={"seq": other},
            device_id_type=MESH,
        )

    def finish(n):
        swap(n).wait_recv()
        at = pl.ds(n * rows_of, rows_of)
        mine = part[at, pl.ds(pl.multiple_of(seq * hj, hj), hj), :]
        out_ref[at] = (mine + got[at] + bias_ref[...][None]).astype(BF16)

    def tail(n, _):
        unit(PHASES - 1, n)
        for ii in range(rows_of):
            i = n * rows_of + ii
            tile = acc[:, pl.ds(pl.multiple_of(i * nj, nj), nj)] * scale_ref[pl.ds(i, 1), :]
            part[pl.ds(i, 1)] = tile.T[None]
        swap(n).start()

        @pl.when(n >= 2)
        def _():
            finish(n - 2)

        return 0

    lax.fori_loop(0, units, tail, 0)
    finish(units - 2)
    finish(units - 1)
    for n in range(units):
        swap(n).wait_send()
    for ph in range(PHASES):
        for way in (0, 1):
            for t in range(1, steps(way, ph) + 1):
                for kind in (0, 1):
                    ring(way, ph, t, kind).wait_send()


def body(sizes, pl_, pr, ul, ur, weight, bias, lengths, depths):
    nrow, ncol, nseq = sizes
    chans, ni = pl_.shape[1], pl_.shape[2]
    nj = pr.shape[2]
    nz = weight.shape[1]
    s_paired = float(pr.shape[0] * nrow * nseq)
    dims = (nrow, ncol, nseq, chans, lengths.shape[0], ni, nj, nz, s_paired)
    half = nrow // 2
    tall = ni * chans
    vm = pl.BlockSpec(memory_space=pltpu.VMEM)
    hbm = pl.BlockSpec(memory_space=pltpu.HBM)
    sm = pl.BlockSpec(memory_space=pltpu.SMEM)
    dma = pltpu.SemaphoreType.DMA
    hj = nj // nseq
    return pl.pallas_call(
        functools.partial(kernel, dims),
        out_shape=jax.ShapeDtypeStruct((ni, hj, nz), BF16),
        in_specs=[hbm] * 5 + [vm] + [sm] * 2,
        out_specs=vm,
        scratch_shapes=[
            pltpu.VMEM(pr.shape, BF16),
            pltpu.VMEM(ur.shape, BF16),
            pltpu.VMEM((chans, ni, pl_.shape[0]), BF16),
            pltpu.VMEM((chans, ni, ul.shape[0]), BF16),
            pltpu.VMEM(weight.shape, BF16),
            pltpu.VMEM((tall, tall), BF16),
            pltpu.VMEM((nz, tall), BF16),
            pltpu.VMEM((nrow, pr.shape[0], chans * nj), BF16),
            pltpu.VMEM((nrow, ur.shape[0], chans * nj), BF16),
            pltpu.VMEM((ncol, pl_.shape[0], tall), BF16),
            pltpu.VMEM((tall, ncol * pl_.shape[0]), BF16),
            pltpu.VMEM((tall, ncol * ul.shape[0]), BF16),
            pltpu.VMEM((nz, ni * nj), F32),
            pltpu.VMEM((ni, nj, nz), F32),
            pltpu.VMEM((ni, hj, nz), F32),
            pltpu.VMEM((ni, nj), F32),
            pltpu.VMEM((ni, nj), F32),
            dma((2 * PHASES * half * 2,)),
            dma((2 * PHASES * half * 2,)),
            dma(((ncol - 1) * 2,)),
            dma(((ncol - 1) * 2,)),
            dma((ni // ROWS_PER_UNIT,)),
            dma((ni // ROWS_PER_UNIT,)),
            dma((5,)),
        ],
        compiler_params=pltpu.CompilerParams(
            collective_id=0, has_side_effects=True, vmem_limit_bytes=67043328
        ),
    )(
        pr,
        ur,
        jnp.transpose(pl_, (1, 2, 0)),
        jnp.transpose(ul, (1, 2, 0)),
        weight,
        bias.reshape(1, nz),
        lengths,
        depths,
    )


def solution(mesh):
    sizes = (mesh.shape["row"], mesh.shape["col"], mesh.shape["seq"])
    return jax.shard_map(
        functools.partial(body, sizes),
        mesh=mesh,
        in_specs=(
            P(("groups", "seq", "col"), None, "row"),
            P(("groups", "seq", "row"), None, "col"),
            P(("groups", "seq", "col"), None, "row"),
            P(("groups", "seq", "row"), None, "col"),
            P(),
            P(),
            P("groups"),
            P("groups"),
        ),
        out_specs=P(("groups", "row"), ("col", "seq"), None),
        check_vma=False,
    )
```

```python
import functools

import jax
import jax.numpy as jnp
from jax import lax
from jax.experimental import pallas as pl
from jax.experimental.pallas import tpu as pltpu
from jax.sharding import PartitionSpec as P

MESH = pl.DeviceIdType.MESH
F32 = jnp.float32
BF16 = jnp.bfloat16
PHASES = 4
I_UNIT = 16
TAIL_UNIT = 8


def kernel(
    dims,
    pr_ref,
    ur_ref,
    pl_ref,
    ul_ref,
    w_ref,
    bias_ref,
    len_ref,
    dep_ref,
    out_ref,
    prv,
    urv,
    plv,
    ulv,
    wv,
    perm,
    wt_ref,
    rbp,
    rbu,
    lbp,
    ltp,
    ltu,
    acc,
    part,
    got,
    same_ref,
    scale_ref,
    send_r,
    recv_r,
    send_l,
    recv_l,
    send_x,
    recv_x,
    load_sem,
):
    nrow, ncol, nseq, chans, chains, ni, nj, nz, s_paired = dims
    me = lax.axis_index("row")
    col = lax.axis_index("col")
    seq = lax.axis_index("seq")
    right, left = lax.rem(me + 1, nrow), lax.rem(me + nrow - 1, nrow)
    other = 1 - seq
    lanes = chans * nj // PHASES
    per_phase = chans // PHASES

    loads = [
        pltpu.make_async_copy(src, dst, load_sem.at[k])
        for k, (src, dst) in enumerate(
            ((pr_ref, prv), (ur_ref, urv), (pl_ref, plv), (ul_ref, ulv), (w_ref, wv))
        )
    ]
    for load in loads:
        load.start()

    barrier = pltpu.get_barrier_semaphore()
    for nb in (right, left):
        pl.semaphore_signal(barrier, inc=1, device_id={"row": nb}, device_id_type=MESH)
    for k in range(1, ncol):
        pl.semaphore_signal(
            barrier, inc=1, device_id={"col": lax.rem(col + k, ncol)}, device_id_type=MESH
        )
    pl.semaphore_signal(barrier, inc=1, device_id={"seq": other}, device_id_type=MESH)
    loads[0].wait()
    rbp[pl.ds(me, 1)] = prv[...].reshape(1, -1, chans * nj)
    loads[1].wait()
    rbu[pl.ds(me, 1)] = urv[...].reshape(1, -1, chans * nj)
    pl.semaphore_wait(barrier, 2 + ncol - 1 + 1)

    half = nrow // 2

    def steps(way, ph):
        return half if (ph + way) % 2 == 0 else half - 1

    def block(way, t):
        return lax.rem(me - t + nrow, nrow) if way == 0 else lax.rem(me + t, nrow)

    def ring(way, ph, t, kind):
        q = block(way, t - 1)
        buf = (rbp, rbu)[kind]
        part_of = pl.ds(ph * lanes, lanes)
        at = ((way * PHASES + ph) * half + t - 1) * 2 + kind
        return pltpu.make_async_remote_copy(
            src_ref=buf.at[q, :, part_of],
            dst_ref=buf.at[q, :, part_of],
            send_sem=send_r.at[at],
            recv_sem=recv_r.at[at],
            device_id={"row": right if way == 0 else left},
            device_id_type=MESH,
        )

    def arrival(way, ph, t, kind):
        q = block(way, t)
        buf = (rbp, rbu)[kind]
        part_of = pl.ds(ph * lanes, lanes)
        at = ((way * PHASES + ph) * half + t - 1) * 2 + kind
        return pltpu.make_async_remote_copy(
            src_ref=buf.at[q, :, part_of],
            dst_ref=buf.at[q, :, part_of],
            send_sem=send_r.at[at],
            recv_sem=recv_r.at[at],
            device_id={"row": right if way == 0 else left},
            device_id_type=MESH,
        )

    def first_sends(ph):
        for kind in (1, 0):
            for way in (0, 1):
                ring(way, ph, 1, kind).start()

    tall = ni * chans
    lu_rows = ulv.shape[2]

    def left_copy(k, kind, incoming):
        at = (k - 1) * 2 + kind
        slot = lax.rem(col - k + ncol, ncol) if incoming else col
        if kind == 0:
            src = dst = lbp.at[slot]
        else:
            src = dst = ltu.at[:, pl.ds(pl.multiple_of(slot * lu_rows, lu_rows), lu_rows)]
        return pltpu.make_async_remote_copy(
            src_ref=src,
            dst_ref=dst,
            send_sem=send_l.at[at],
            recv_sem=recv_l.at[at],
            device_id={"col": lax.rem(col + k, ncol)},
            device_id_type=MESH,
        )

    first_sends(0)

    block_rows = 128

    def fill(b, _):
        rows = pl.ds(pl.multiple_of(b * block_rows, block_rows), block_rows)
        r = lax.broadcasted_iota(jnp.int32, (block_rows, tall), 0) + b * block_rows
        k = lax.broadcasted_iota(jnp.int32, (block_rows, tall), 1)
        hit = k == (r % chans) * chans + r // chans
        perm[rows, :] = jnp.where(hit, 1.0, 0.0).astype(BF16)
        return 0

    lax.fori_loop(0, tall // block_rows, fill, 0)
    for load in loads[2:]:
        load.wait()
    lbp[pl.ds(col, 1)] = lax.dot_general(
        plv[...].reshape(tall, -1), perm[...], (((0,), (1,)), ((), ())),
        preferred_element_type=F32,
    ).astype(BF16)[None]
    ltu[:, pl.ds(pl.multiple_of(col * lu_rows, lu_rows), lu_rows)] = jnp.dot(
        perm[...], ulv[...].reshape(tall, -1), preferred_element_type=F32
    ).astype(BF16)
    for k in range(1, ncol):
        for kind in (0, 1):
            left_copy(k, kind, False).start()
    wt_ref[...] = jnp.dot(perm[...], wv[...], preferred_element_type=F32).T.astype(BF16)

    pos_i = lax.broadcasted_iota(jnp.int32, (ni, nj), 0) + me * ni
    pos_j = lax.broadcasted_iota(jnp.int32, (ni, nj), 1) + col * nj
    chain_i = jnp.zeros((ni, nj), jnp.int32)
    chain_j = jnp.zeros((ni, nj), jnp.int32)
    end = jnp.int32(0)
    ends = []
    for k in range(chains):
        end = end + len_ref[k]
        ends.append(end)
        chain_i = chain_i + (pos_i >= end).astype(jnp.int32)
        chain_j = chain_j + (pos_j >= end).astype(jnp.int32)
    same = (chain_i == chain_j).astype(F32)
    depth_i = jnp.zeros((ni, nj), F32)
    for k in range(chains):
        depth_i = depth_i + jnp.where(chain_i == k, dep_ref[k].astype(F32), 0.0)
    same_ref[...] = same
    scale_ref[...] = 1.0 / (s_paired + same * depth_i)

    def forward(ph, t):
        for kind in (1, 0):
            for way in (0, 1):
                if t <= steps(way, ph):
                    arrival(way, ph, t, kind).wait_recv()
                    if t < steps(way, ph):
                        ring(way, ph, t + 1, kind).start()

    free_rows = ltu.shape[1]

    def left_ready():
        for k in range(1, ncol):
            for kind in (0, 1):
                left_copy(k, kind, True).wait_recv()
        for k in range(1, ncol):
            for kind in (0, 1):
                left_copy(k, kind, False).wait_send()
        ltp[...] = lbp[...].reshape(-1, tall).T

        def mask_rows(b, _):
            rows = pl.ds(pl.multiple_of(b * block_rows, block_rows), block_rows)
            shape = (block_rows, nj)
            pos = (lax.broadcasted_iota(jnp.int32, shape, 0) + b * block_rows) // chans + me * ni
            ids = lax.broadcasted_iota(jnp.int32, shape, 1) + seq * free_rows
            depth = jnp.zeros(shape, jnp.int32)
            for k in range(chains):
                low = ends[k - 1] if k else 0
                depth = jnp.where((pos >= low) & (pos < ends[k]), dep_ref[k], depth)
            for at in range(0, free_rows, nj):
                live = jnp.where(ids + at < depth, 1.0, 0.0).astype(BF16)
                ltu[rows, at : at + nj] = ltu[rows, at : at + nj] * live
            return 0

        lax.fori_loop(0, ni * chans // block_rows, mask_rows, 0)

    def unit(ph, base, count):
        rows = count * chans
        at = pl.ds(pl.multiple_of(base * chans, rows), rows)
        part_of = pl.ds(ph * lanes, lanes)
        kp = rbp.shape[0] * rbp.shape[1]
        ku = rbu.shape[0] * rbu.shape[1]
        a = jnp.dot(ltp[at, :], rbp[:, :, part_of].reshape(kp, lanes), preferred_element_type=F32)
        b = jnp.dot(ltu[at, :], rbu[:, :, part_of].reshape(ku, lanes), preferred_element_type=F32)
        w = wt_ref[:, ph * per_phase * chans : (ph + 1) * per_phase * chans]
        for pair in range(count // 2):
            cols = []
            for ii in (2 * pair, 2 * pair + 1):
                m = same_ref[pl.ds(base + ii, 1), :]
                tiles = []
                for d in range(per_phase):
                    rs = slice(ii * chans, (ii + 1) * chans)
                    ls = slice(d * nj, (d + 1) * nj)
                    tiles.append((a[rs, ls] + b[rs, ls] * m).astype(BF16))
                cols.append(jnp.concatenate(tiles, axis=0))
            x = jnp.concatenate(cols, axis=1)
            to = pl.ds(pl.multiple_of((base + 2 * pair) * nj, 2 * nj), 2 * nj)
            y = jnp.dot(w, x, preferred_element_type=F32)
            if ph == 0:
                acc[:, to] = y
            else:
                acc[:, to] += y

    def whole(ph):
        def one(n, _):
            unit(ph, n * I_UNIT, I_UNIT)
            return 0

        lax.fori_loop(0, ni // I_UNIT, one, 0)

    first_sends(1)
    for t in range(1, half + 1):
        for ph in (0, 1):
            forward(ph, t)
        if t == half - 1:
            first_sends(2)
            first_sends(3)
        if t == half // 2:
            left_ready()
    for t in range(1, half + 1):
        for ph in (2, 3):
            forward(ph, t)
            if t == half and ph == 2:
                whole(2)
        if t in (1, 2):
            whole(t - 1)

    hj = nj // nseq
    rows_of = TAIL_UNIT
    units = ni // rows_of

    def swap(n):
        at = pl.ds(n * rows_of, rows_of)
        return pltpu.make_async_remote_copy(
            src_ref=part.at[at, pl.ds(pl.multiple_of(other * hj, hj), hj), :],
            dst_ref=got.at[at],
            send_sem=send_x.at[n],
            recv_sem=recv_x.at[n],
            device_id={"seq": other},
            device_id_type=MESH,
        )

    def finish(n):
        swap(n).wait_recv()
        at = pl.ds(n * rows_of, rows_of)
        mine = part[at, pl.ds(pl.multiple_of(seq * hj, hj), hj), :]
        out_ref[at] = (mine + got[at] + bias_ref[...][None]).astype(BF16)

    def tail(n, _):
        unit(PHASES - 1, n * rows_of, rows_of)
        for ii in range(rows_of):
            i = n * rows_of + ii
            tile = acc[:, pl.ds(pl.multiple_of(i * nj, nj), nj)] * scale_ref[pl.ds(i, 1), :]
            part[pl.ds(i, 1)] = tile.T[None]
        swap(n).start()

        @pl.when(n >= 1)
        def _():
            finish(n - 1)

        return 0

    lax.fori_loop(0, units, tail, 0)
    finish(units - 1)
    for n in range(units):
        swap(n).wait_send()
    for ph in range(PHASES):
        for way in (0, 1):
            for t in range(1, steps(way, ph) + 1):
                for kind in (0, 1):
                    ring(way, ph, t, kind).wait_send()


def body(sizes, pl_, pr, ul, ur, weight, bias, lengths, depths):
    nrow, ncol, nseq = sizes
    chans, ni = pl_.shape[1], pl_.shape[2]
    nj = pr.shape[2]
    nz = weight.shape[1]
    s_paired = float(pr.shape[0] * nrow * nseq)
    dims = (nrow, ncol, nseq, chans, lengths.shape[0], ni, nj, nz, s_paired)
    half = nrow // 2
    tall = ni * chans
    vm = pl.BlockSpec(memory_space=pltpu.VMEM)
    hbm = pl.BlockSpec(memory_space=pltpu.HBM)
    sm = pl.BlockSpec(memory_space=pltpu.SMEM)
    dma = pltpu.SemaphoreType.DMA
    hj = nj // nseq
    return pl.pallas_call(
        functools.partial(kernel, dims),
        out_shape=jax.ShapeDtypeStruct((ni, hj, nz), BF16),
        in_specs=[hbm] * 5 + [vm] + [sm] * 2,
        out_specs=vm,
        scratch_shapes=[
            pltpu.VMEM(pr.shape, BF16),
            pltpu.VMEM(ur.shape, BF16),
            pltpu.VMEM((chans, ni, pl_.shape[0]), BF16),
            pltpu.VMEM((chans, ni, ul.shape[0]), BF16),
            pltpu.VMEM(weight.shape, BF16),
            pltpu.VMEM((tall, tall), BF16),
            pltpu.VMEM((nz, tall), BF16),
            pltpu.VMEM((nrow, pr.shape[0], chans * nj), BF16),
            pltpu.VMEM((nrow, ur.shape[0], chans * nj), BF16),
            pltpu.VMEM((ncol, pl_.shape[0], tall), BF16),
            pltpu.VMEM((tall, ncol * pl_.shape[0]), BF16),
            pltpu.VMEM((tall, ncol * ul.shape[0]), BF16),
            pltpu.VMEM((nz, ni * nj), F32),
            pltpu.VMEM((ni, nj, nz), F32),
            pltpu.VMEM((ni, hj, nz), F32),
            pltpu.VMEM((ni, nj), F32),
            pltpu.VMEM((ni, nj), F32),
            dma((2 * PHASES * half * 2,)),
            dma((2 * PHASES * half * 2,)),
            dma(((ncol - 1) * 2,)),
            dma(((ncol - 1) * 2,)),
            dma((ni // TAIL_UNIT,)),
            dma((ni // TAIL_UNIT,)),
            dma((5,)),
        ],
        compiler_params=pltpu.CompilerParams(
            collective_id=0, has_side_effects=True, vmem_limit_bytes=67043328 - 600 * 1024
        ),
    )(
        pr,
        ur,
        jnp.transpose(pl_, (1, 2, 0)),
        jnp.transpose(ul, (1, 2, 0)),
        weight,
        bias.reshape(1, nz),
        lengths,
        depths,
    )


def solution(mesh):
    sizes = (mesh.shape["row"], mesh.shape["col"], mesh.shape["seq"])
    return jax.shard_map(
        functools.partial(body, sizes),
        mesh=mesh,
        in_specs=(
            P(("groups", "seq", "col"), None, "row"),
            P(("groups", "seq", "row"), None, "col"),
            P(("groups", "seq", "col"), None, "row"),
            P(("groups", "seq", "row"), None, "col"),
            P(),
            P(),
            P("groups"),
            P("groups"),
        ),
        out_specs=P(("groups", "row"), ("col", "seq"), None),
        check_vma=False,
    )
```

```python
import functools

import jax
import jax.numpy as jnp
from jax import lax
from jax.experimental import pallas as pl
from jax.experimental.pallas import tpu as pltpu
from jax.sharding import PartitionSpec as P

MESH = pl.DeviceIdType.MESH
F32 = jnp.float32
BF16 = jnp.bfloat16
PHASES = 4
I_UNIT = 16
TAIL_UNIT = 8


def kernel(
    dims,
    pr_ref,
    ur_ref,
    pl_ref,
    ul_ref,
    w_ref,
    bias_ref,
    len_ref,
    dep_ref,
    out_ref,
    prv,
    urv,
    plv,
    ulv,
    wv,
    perm,
    wt_ref,
    rbp,
    rbu,
    lbp,
    ltp,
    ltu,
    acc,
    part,
    got,
    same_ref,
    scale_ref,
    send_r,
    recv_r,
    send_l,
    recv_l,
    send_x,
    recv_x,
    load_sem,
):
    nrow, ncol, nseq, chans, chains, ni, nj, nz, s_paired = dims
    me = lax.axis_index("row")
    col = lax.axis_index("col")
    seq = lax.axis_index("seq")
    right, left = lax.rem(me + 1, nrow), lax.rem(me + nrow - 1, nrow)
    other = 1 - seq
    lanes = chans * nj // PHASES
    per_phase = chans // PHASES

    loads = [
        pltpu.make_async_copy(src, dst, load_sem.at[k])
        for k, (src, dst) in enumerate(
            ((pr_ref, prv), (ur_ref, urv), (pl_ref, plv), (ul_ref, ulv), (w_ref, wv))
        )
    ]
    for load in loads:
        load.start()

    barrier = pltpu.get_barrier_semaphore()
    for nb in (right, left):
        pl.semaphore_signal(barrier, inc=1, device_id={"row": nb}, device_id_type=MESH)
    for k in range(1, ncol):
        pl.semaphore_signal(
            barrier, inc=1, device_id={"col": lax.rem(col + k, ncol)}, device_id_type=MESH
        )
    pl.semaphore_signal(barrier, inc=1, device_id={"seq": other}, device_id_type=MESH)
    loads[0].wait()
    rbp[pl.ds(me, 1)] = prv[...].reshape(1, -1, chans * nj)
    loads[1].wait()
    rbu[pl.ds(me, 1)] = urv[...].reshape(1, -1, chans * nj)
    pl.semaphore_wait(barrier, 2 + ncol - 1 + 1)

    half = nrow // 2

    def steps(way, ph):
        return half if (ph + way) % 2 == 0 else half - 1

    def block(way, t):
        return lax.rem(me - t + nrow, nrow) if way == 0 else lax.rem(me + t, nrow)

    def ring(way, ph, t, kind):
        q = block(way, t - 1)
        buf = (rbp, rbu)[kind]
        part_of = pl.ds(ph * lanes, lanes)
        at = ((way * PHASES + ph) * half + t - 1) * 2 + kind
        return pltpu.make_async_remote_copy(
            src_ref=buf.at[q, :, part_of],
            dst_ref=buf.at[q, :, part_of],
            send_sem=send_r.at[at],
            recv_sem=recv_r.at[at],
            device_id={"row": right if way == 0 else left},
            device_id_type=MESH,
        )

    def arrival(way, ph, t, kind):
        q = block(way, t)
        buf = (rbp, rbu)[kind]
        part_of = pl.ds(ph * lanes, lanes)
        at = ((way * PHASES + ph) * half + t - 1) * 2 + kind
        return pltpu.make_async_remote_copy(
            src_ref=buf.at[q, :, part_of],
            dst_ref=buf.at[q, :, part_of],
            send_sem=send_r.at[at],
            recv_sem=recv_r.at[at],
            device_id={"row": right if way == 0 else left},
            device_id_type=MESH,
        )

    def first_sends(ph):
        for kind in (1, 0):
            for way in (0, 1):
                ring(way, ph, 1, kind).start()

    tall = ni * chans
    lu_rows = ulv.shape[2]

    def left_copy(k, kind, incoming):
        at = (k - 1) * 2 + kind
        slot = lax.rem(col - k + ncol, ncol) if incoming else col
        if kind == 0:
            src = dst = lbp.at[slot]
        else:
            src = dst = ltu.at[:, pl.ds(pl.multiple_of(slot * lu_rows, lu_rows), lu_rows)]
        return pltpu.make_async_remote_copy(
            src_ref=src,
            dst_ref=dst,
            send_sem=send_l.at[at],
            recv_sem=recv_l.at[at],
            device_id={"col": lax.rem(col + k, ncol)},
            device_id_type=MESH,
        )

    first_sends(0)
    first_sends(1)

    block_rows = 128

    def fill(b, _):
        rows = pl.ds(pl.multiple_of(b * block_rows, block_rows), block_rows)
        r = lax.broadcasted_iota(jnp.int32, (block_rows, tall), 0) + b * block_rows
        k = lax.broadcasted_iota(jnp.int32, (block_rows, tall), 1)
        hit = k == (r % chans) * chans + r // chans
        perm[rows, :] = jnp.where(hit, 1.0, 0.0).astype(BF16)
        return 0

    lax.fori_loop(0, tall // block_rows, fill, 0)
    for load in loads[2:]:
        load.wait()
    lbp[pl.ds(col, 1)] = lax.dot_general(
        plv[...].reshape(tall, -1), perm[...], (((0,), (1,)), ((), ())),
        preferred_element_type=F32,
    ).astype(BF16)[None]
    ltu[:, pl.ds(pl.multiple_of(col * lu_rows, lu_rows), lu_rows)] = jnp.dot(
        perm[...], ulv[...].reshape(tall, -1), preferred_element_type=F32
    ).astype(BF16)
    for k in range(1, ncol):
        for kind in (0, 1):
            left_copy(k, kind, False).start()
    wt_ref[...] = jnp.dot(perm[...], wv[...], preferred_element_type=F32).T.astype(BF16)

    pos_i = lax.broadcasted_iota(jnp.int32, (ni, nj), 0) + me * ni
    pos_j = lax.broadcasted_iota(jnp.int32, (ni, nj), 1) + col * nj
    chain_i = jnp.zeros((ni, nj), jnp.int32)
    chain_j = jnp.zeros((ni, nj), jnp.int32)
    end = jnp.int32(0)
    ends = []
    for k in range(chains):
        end = end + len_ref[k]
        ends.append(end)
        chain_i = chain_i + (pos_i >= end).astype(jnp.int32)
        chain_j = chain_j + (pos_j >= end).astype(jnp.int32)
    same = (chain_i == chain_j).astype(F32)
    depth_i = jnp.zeros((ni, nj), F32)
    for k in range(chains):
        depth_i = depth_i + jnp.where(chain_i == k, dep_ref[k].astype(F32), 0.0)
    same_ref[...] = same
    scale_ref[...] = 1.0 / (s_paired + same * depth_i)

    def forward(ph, t):
        for kind in (1, 0):
            for way in (0, 1):
                if t <= steps(way, ph):
                    arrival(way, ph, t, kind).wait_recv()
                    if t < steps(way, ph):
                        ring(way, ph, t + 1, kind).start()

    free_rows = ltu.shape[1]

    def left_ready():
        for k in range(1, ncol):
            for kind in (0, 1):
                left_copy(k, kind, True).wait_recv()
        for k in range(1, ncol):
            for kind in (0, 1):
                left_copy(k, kind, False).wait_send()
        ltp[...] = lbp[...].reshape(-1, tall).T

        def mask_rows(b, _):
            rows = pl.ds(pl.multiple_of(b * block_rows, block_rows), block_rows)
            shape = (block_rows, nj)
            pos = (lax.broadcasted_iota(jnp.int32, shape, 0) + b * block_rows) // chans + me * ni
            ids = lax.broadcasted_iota(jnp.int32, shape, 1) + seq * free_rows
            depth = jnp.zeros(shape, jnp.int32)
            for k in range(chains):
                low = ends[k - 1] if k else 0
                depth = jnp.where((pos >= low) & (pos < ends[k]), dep_ref[k], depth)
            for at in range(0, free_rows, nj):
                live = jnp.where(ids + at < depth, 1.0, 0.0).astype(BF16)
                ltu[rows, at : at + nj] = ltu[rows, at : at + nj] * live
            return 0

        lax.fori_loop(0, ni * chans // block_rows, mask_rows, 0)

    def unit(ph, base, count):
        rows = count * chans
        at = pl.ds(pl.multiple_of(base * chans, rows), rows)
        part_of = pl.ds(ph * lanes, lanes)
        kp = rbp.shape[0] * rbp.shape[1]
        ku = rbu.shape[0] * rbu.shape[1]
        a = jnp.dot(ltp[at, :], rbp[:, :, part_of].reshape(kp, lanes), preferred_element_type=F32)
        b = jnp.dot(ltu[at, :], rbu[:, :, part_of].reshape(ku, lanes), preferred_element_type=F32)
        w = wt_ref[:, ph * per_phase * chans : (ph + 1) * per_phase * chans]
        for pair in range(count // 2):
            cols = []
            for ii in (2 * pair, 2 * pair + 1):
                m = same_ref[pl.ds(base + ii, 1), :]
                tiles = []
                for d in range(per_phase):
                    rs = slice(ii * chans, (ii + 1) * chans)
                    ls = slice(d * nj, (d + 1) * nj)
                    tiles.append((a[rs, ls] + b[rs, ls] * m).astype(BF16))
                cols.append(jnp.concatenate(tiles, axis=0))
            x = jnp.concatenate(cols, axis=1)
            to = pl.ds(pl.multiple_of((base + 2 * pair) * nj, 2 * nj), 2 * nj)
            y = jnp.dot(w, x, preferred_element_type=F32)
            if ph == 0:
                acc[:, to] = y
            else:
                acc[:, to] += y

    def whole(ph):
        def one(n, _):
            unit(ph, n * I_UNIT, I_UNIT)
            return 0

        lax.fori_loop(0, ni // I_UNIT, one, 0)

    lag = 2
    for slot in range(1, half + lag + 1):
        for ph in range(PHASES):
            t = slot - (lag if ph >= 2 else 0)
            if 1 <= t <= half:
                forward(ph, t)
            if slot == half + lag and ph == 2:
                whole(2)
        if slot == lag:
            first_sends(2)
            first_sends(3)
        if slot == half // 2:
            left_ready()
        if slot == half:
            whole(0)
        if slot == half + 1:
            whole(1)

    hj = nj // nseq
    rows_of = TAIL_UNIT
    units = ni // rows_of

    def swap(n):
        at = pl.ds(n * rows_of, rows_of)
        return pltpu.make_async_remote_copy(
            src_ref=part.at[at, pl.ds(pl.multiple_of(other * hj, hj), hj), :],
            dst_ref=got.at[at],
            send_sem=send_x.at[n],
            recv_sem=recv_x.at[n],
            device_id={"seq": other},
            device_id_type=MESH,
        )

    def finish(n):
        swap(n).wait_recv()
        at = pl.ds(n * rows_of, rows_of)
        mine = part[at, pl.ds(pl.multiple_of(seq * hj, hj), hj), :]
        out_ref[at] = (mine + got[at] + bias_ref[...][None]).astype(BF16)

    def tail(n, _):
        unit(PHASES - 1, n * rows_of, rows_of)
        for ii in range(rows_of):
            i = n * rows_of + ii
            tile = acc[:, pl.ds(pl.multiple_of(i * nj, nj), nj)] * scale_ref[pl.ds(i, 1), :]
            part[pl.ds(i, 1)] = tile.T[None]
        swap(n).start()

        @pl.when(n >= 1)
        def _():
            finish(n - 1)

        return 0

    lax.fori_loop(0, units, tail, 0)
    finish(units - 1)
    for n in range(units):
        swap(n).wait_send()
    for ph in range(PHASES):
        for way in (0, 1):
            for t in range(1, steps(way, ph) + 1):
                for kind in (0, 1):
                    ring(way, ph, t, kind).wait_send()


def body(sizes, pl_, pr, ul, ur, weight, bias, lengths, depths):
    nrow, ncol, nseq = sizes
    chans, ni = pl_.shape[1], pl_.shape[2]
    nj = pr.shape[2]
    nz = weight.shape[1]
    s_paired = float(pr.shape[0] * nrow * nseq)
    dims = (nrow, ncol, nseq, chans, lengths.shape[0], ni, nj, nz, s_paired)
    half = nrow // 2
    tall = ni * chans
    vm = pl.BlockSpec(memory_space=pltpu.VMEM)
    hbm = pl.BlockSpec(memory_space=pltpu.HBM)
    sm = pl.BlockSpec(memory_space=pltpu.SMEM)
    dma = pltpu.SemaphoreType.DMA
    hj = nj // nseq
    return pl.pallas_call(
        functools.partial(kernel, dims),
        out_shape=jax.ShapeDtypeStruct((ni, hj, nz), BF16),
        in_specs=[hbm] * 5 + [vm] + [sm] * 2,
        out_specs=vm,
        scratch_shapes=[
            pltpu.VMEM(pr.shape, BF16),
            pltpu.VMEM(ur.shape, BF16),
            pltpu.VMEM((chans, ni, pl_.shape[0]), BF16),
            pltpu.VMEM((chans, ni, ul.shape[0]), BF16),
            pltpu.VMEM(weight.shape, BF16),
            pltpu.VMEM((tall, tall), BF16),
            pltpu.VMEM((nz, tall), BF16),
            pltpu.VMEM((nrow, pr.shape[0], chans * nj), BF16),
            pltpu.VMEM((nrow, ur.shape[0], chans * nj), BF16),
            pltpu.VMEM((ncol, pl_.shape[0], tall), BF16),
            pltpu.VMEM((tall, ncol * pl_.shape[0]), BF16),
            pltpu.VMEM((tall, ncol * ul.shape[0]), BF16),
            pltpu.VMEM((nz, ni * nj), F32),
            pltpu.VMEM((ni, nj, nz), F32),
            pltpu.VMEM((ni, hj, nz), F32),
            pltpu.VMEM((ni, nj), F32),
            pltpu.VMEM((ni, nj), F32),
            dma((2 * PHASES * half * 2,)),
            dma((2 * PHASES * half * 2,)),
            dma(((ncol - 1) * 2,)),
            dma(((ncol - 1) * 2,)),
            dma((ni // TAIL_UNIT,)),
            dma((ni // TAIL_UNIT,)),
            dma((5,)),
        ],
        compiler_params=pltpu.CompilerParams(
            collective_id=0, has_side_effects=True, vmem_limit_bytes=67043328 - 600 * 1024
        ),
    )(
        pr,
        ur,
        jnp.transpose(pl_, (1, 2, 0)),
        jnp.transpose(ul, (1, 2, 0)),
        weight,
        bias.reshape(1, nz),
        lengths,
        depths,
    )


def solution(mesh):
    sizes = (mesh.shape["row"], mesh.shape["col"], mesh.shape["seq"])
    return jax.shard_map(
        functools.partial(body, sizes),
        mesh=mesh,
        in_specs=(
            P(("groups", "seq", "col"), None, "row"),
            P(("groups", "seq", "row"), None, "col"),
            P(("groups", "seq", "col"), None, "row"),
            P(("groups", "seq", "row"), None, "col"),
            P(),
            P(),
            P("groups"),
            P("groups"),
        ),
        out_specs=P(("groups", "row"), ("col", "seq"), None),
        check_vma=False,
    )
```

```python
import functools

import jax
import jax.numpy as jnp
from jax import lax
from jax.experimental import pallas as pl
from jax.experimental.pallas import tpu as pltpu
from jax.sharding import PartitionSpec as P

MESH = pl.DeviceIdType.MESH
F32 = jnp.float32
BF16 = jnp.bfloat16
PHASES = 4
I_UNIT = 32
TAIL_UNIT = 8


def kernel(
    dims,
    pr_ref,
    ur_ref,
    pl_ref,
    ul_ref,
    w_ref,
    bias_ref,
    len_ref,
    dep_ref,
    out_ref,
    prv,
    urv,
    plv,
    ulv,
    wv,
    perm,
    wt_ref,
    rbp,
    rbu,
    lbp,
    ltp,
    ltu,
    acc,
    part,
    got,
    same_ref,
    scale_ref,
    send_r,
    recv_r,
    send_l,
    recv_l,
    send_x,
    recv_x,
    load_sem,
):
    nrow, ncol, nseq, chans, chains, ni, nj, nz, s_paired = dims
    me = lax.axis_index("row")
    col = lax.axis_index("col")
    seq = lax.axis_index("seq")
    right, left = lax.rem(me + 1, nrow), lax.rem(me + nrow - 1, nrow)
    other = 1 - seq
    lanes = chans * nj // PHASES
    per_phase = chans // PHASES

    loads = [
        pltpu.make_async_copy(src, dst, load_sem.at[k])
        for k, (src, dst) in enumerate(
            ((pr_ref, prv), (ur_ref, urv), (pl_ref, plv), (ul_ref, ulv), (w_ref, wv))
        )
    ]
    for load in loads:
        load.start()

    barrier = pltpu.get_barrier_semaphore()
    for nb in (right, left):
        pl.semaphore_signal(barrier, inc=1, device_id={"row": nb}, device_id_type=MESH)
    for k in range(1, ncol):
        pl.semaphore_signal(
            barrier, inc=1, device_id={"col": lax.rem(col + k, ncol)}, device_id_type=MESH
        )
    pl.semaphore_signal(barrier, inc=1, device_id={"seq": other}, device_id_type=MESH)
    loads[0].wait()
    rbp[pl.ds(me, 1)] = prv[...].reshape(1, -1, chans * nj)
    loads[1].wait()
    rbu[pl.ds(me, 1)] = urv[...].reshape(1, -1, chans * nj)
    pl.semaphore_wait(barrier, 2 + ncol - 1 + 1)

    half = nrow // 2

    def steps(way, ph):
        return half if (ph + way) % 2 == 0 else half - 1

    def block(way, t):
        return lax.rem(me - t + nrow, nrow) if way == 0 else lax.rem(me + t, nrow)

    def ring(way, ph, t, kind):
        q = block(way, t - 1)
        buf = (rbp, rbu)[kind]
        part_of = pl.ds(ph * lanes, lanes)
        at = ((way * PHASES + ph) * half + t - 1) * 2 + kind
        return pltpu.make_async_remote_copy(
            src_ref=buf.at[q, :, part_of],
            dst_ref=buf.at[q, :, part_of],
            send_sem=send_r.at[at],
            recv_sem=recv_r.at[at],
            device_id={"row": right if way == 0 else left},
            device_id_type=MESH,
        )

    def arrival(way, ph, t, kind):
        q = block(way, t)
        buf = (rbp, rbu)[kind]
        part_of = pl.ds(ph * lanes, lanes)
        at = ((way * PHASES + ph) * half + t - 1) * 2 + kind
        return pltpu.make_async_remote_copy(
            src_ref=buf.at[q, :, part_of],
            dst_ref=buf.at[q, :, part_of],
            send_sem=send_r.at[at],
            recv_sem=recv_r.at[at],
            device_id={"row": right if way == 0 else left},
            device_id_type=MESH,
        )

    def first_sends(ph):
        for kind in (1, 0):
            for way in (0, 1):
                ring(way, ph, 1, kind).start()

    tall = ni * chans
    lu_rows = ulv.shape[2]

    def left_copy(k, kind, incoming):
        at = (k - 1) * 2 + kind
        slot = lax.rem(col - k + ncol, ncol) if incoming else col
        if kind == 0:
            src = dst = lbp.at[slot]
        else:
            src = dst = ltu.at[:, pl.ds(pl.multiple_of(slot * lu_rows, lu_rows), lu_rows)]
        return pltpu.make_async_remote_copy(
            src_ref=src,
            dst_ref=dst,
            send_sem=send_l.at[at],
            recv_sem=recv_l.at[at],
            device_id={"col": lax.rem(col + k, ncol)},
            device_id_type=MESH,
        )

    first_sends(0)
    first_sends(1)

    block_rows = 128

    def fill(b, _):
        rows = pl.ds(pl.multiple_of(b * block_rows, block_rows), block_rows)
        r = lax.broadcasted_iota(jnp.int32, (block_rows, tall), 0) + b * block_rows
        k = lax.broadcasted_iota(jnp.int32, (block_rows, tall), 1)
        hit = k == (r % chans) * chans + r // chans
        perm[rows, :] = jnp.where(hit, 1.0, 0.0).astype(BF16)
        return 0

    lax.fori_loop(0, tall // block_rows, fill, 0)
    for load in loads[2:]:
        load.wait()
    lbp[pl.ds(col, 1)] = lax.dot_general(
        plv[...].reshape(tall, -1), perm[...], (((0,), (1,)), ((), ())),
        preferred_element_type=F32,
    ).astype(BF16)[None]
    ltu[:, pl.ds(pl.multiple_of(col * lu_rows, lu_rows), lu_rows)] = jnp.dot(
        perm[...], ulv[...].reshape(tall, -1), preferred_element_type=F32
    ).astype(BF16)
    for k in range(1, ncol):
        for kind in (0, 1):
            left_copy(k, kind, False).start()
    wt_ref[...] = jnp.dot(perm[...], wv[...], preferred_element_type=F32).T.astype(BF16)

    pos_i = lax.broadcasted_iota(jnp.int32, (ni, nj), 0) + me * ni
    pos_j = lax.broadcasted_iota(jnp.int32, (ni, nj), 1) + col * nj
    chain_i = jnp.zeros((ni, nj), jnp.int32)
    chain_j = jnp.zeros((ni, nj), jnp.int32)
    end = jnp.int32(0)
    ends = []
    for k in range(chains):
        end = end + len_ref[k]
        ends.append(end)
        chain_i = chain_i + (pos_i >= end).astype(jnp.int32)
        chain_j = chain_j + (pos_j >= end).astype(jnp.int32)
    same = (chain_i == chain_j).astype(F32)
    depth_i = jnp.zeros((ni, nj), F32)
    for k in range(chains):
        depth_i = depth_i + jnp.where(chain_i == k, dep_ref[k].astype(F32), 0.0)
    same_ref[...] = same
    scale_ref[...] = 1.0 / (s_paired + same * depth_i)

    def forward(ph, t):
        for kind in (1, 0):
            for way in (0, 1):
                if t <= steps(way, ph):
                    arrival(way, ph, t, kind).wait_recv()
                    if t < steps(way, ph):
                        ring(way, ph, t + 1, kind).start()

    free_rows = ltu.shape[1]

    def left_ready():
        for k in range(1, ncol):
            for kind in (0, 1):
                left_copy(k, kind, True).wait_recv()
        for k in range(1, ncol):
            for kind in (0, 1):
                left_copy(k, kind, False).wait_send()
        ltp[...] = lbp[...].reshape(-1, tall).T

        def mask_rows(b, _):
            rows = pl.ds(pl.multiple_of(b * block_rows, block_rows), block_rows)
            shape = (block_rows, nj)
            pos = (lax.broadcasted_iota(jnp.int32, shape, 0) + b * block_rows) // chans + me * ni
            ids = lax.broadcasted_iota(jnp.int32, shape, 1) + seq * free_rows
            depth = jnp.zeros(shape, jnp.int32)
            for k in range(chains):
                low = ends[k - 1] if k else 0
                depth = jnp.where((pos >= low) & (pos < ends[k]), dep_ref[k], depth)
            for at in range(0, free_rows, nj):
                live = jnp.where(ids + at < depth, 1.0, 0.0).astype(BF16)
                ltu[rows, at : at + nj] = ltu[rows, at : at + nj] * live
            return 0

        lax.fori_loop(0, ni * chans // block_rows, mask_rows, 0)

    def unit(ph, base, count):
        rows = count * chans
        at = pl.ds(pl.multiple_of(base * chans, rows), rows)
        part_of = pl.ds(ph * lanes, lanes)
        kp = rbp.shape[0] * rbp.shape[1]
        ku = rbu.shape[0] * rbu.shape[1]
        a = jnp.dot(ltp[at, :], rbp[:, :, part_of].reshape(kp, lanes), preferred_element_type=F32)
        b = jnp.dot(ltu[at, :], rbu[:, :, part_of].reshape(ku, lanes), preferred_element_type=F32)
        w = wt_ref[:, ph * per_phase * chans : (ph + 1) * per_phase * chans]
        for pair in range(count // 2):
            cols = []
            for ii in (2 * pair, 2 * pair + 1):
                m = same_ref[pl.ds(base + ii, 1), :]
                tiles = []
                for d in range(per_phase):
                    rs = slice(ii * chans, (ii + 1) * chans)
                    ls = slice(d * nj, (d + 1) * nj)
                    tiles.append((a[rs, ls] + b[rs, ls] * m).astype(BF16))
                cols.append(jnp.concatenate(tiles, axis=0))
            x = jnp.concatenate(cols, axis=1)
            to = pl.ds(pl.multiple_of((base + 2 * pair) * nj, 2 * nj), 2 * nj)
            y = jnp.dot(w, x, preferred_element_type=F32)
            if ph == 0:
                acc[:, to] = y
            else:
                acc[:, to] += y

    def whole(ph):
        def one(n, _):
            unit(ph, n * I_UNIT, I_UNIT)
            return 0

        lax.fori_loop(0, ni // I_UNIT, one, 0)

    lag = 3
    for slot in range(1, half + lag + 1):
        for ph in range(PHASES):
            t = slot - (lag if ph >= 2 else 0)
            if 1 <= t <= half:
                forward(ph, t)
            if slot == half + lag and ph == 2:
                whole(2)
        if slot == lag:
            first_sends(2)
            first_sends(3)
        if slot == half // 2:
            left_ready()
        if slot == half:
            whole(0)
        if slot == half + 1:
            whole(1)

    hj = nj // nseq
    rows_of = TAIL_UNIT
    units = ni // rows_of

    def swap(n):
        at = pl.ds(n * rows_of, rows_of)
        return pltpu.make_async_remote_copy(
            src_ref=part.at[at, pl.ds(pl.multiple_of(other * hj, hj), hj), :],
            dst_ref=got.at[at],
            send_sem=send_x.at[n],
            recv_sem=recv_x.at[n],
            device_id={"seq": other},
            device_id_type=MESH,
        )

    def finish(n):
        swap(n).wait_recv()
        at = pl.ds(n * rows_of, rows_of)
        mine = part[at, pl.ds(pl.multiple_of(seq * hj, hj), hj), :]
        out_ref[at] = (mine + got[at] + bias_ref[...][None]).astype(BF16)

    def tail(n, _):
        unit(PHASES - 1, n * rows_of, rows_of)
        for ii in range(rows_of):
            i = n * rows_of + ii
            tile = acc[:, pl.ds(pl.multiple_of(i * nj, nj), nj)] * scale_ref[pl.ds(i, 1), :]
            part[pl.ds(i, 1)] = tile.T[None]
        swap(n).start()

        @pl.when(n >= 1)
        def _():
            finish(n - 1)

        return 0

    lax.fori_loop(0, units, tail, 0)
    finish(units - 1)
    for n in range(units):
        swap(n).wait_send()
    for ph in range(PHASES):
        for way in (0, 1):
            for t in range(1, steps(way, ph) + 1):
                for kind in (0, 1):
                    ring(way, ph, t, kind).wait_send()


def body(sizes, pl_, pr, ul, ur, weight, bias, lengths, depths):
    nrow, ncol, nseq = sizes
    chans, ni = pl_.shape[1], pl_.shape[2]
    nj = pr.shape[2]
    nz = weight.shape[1]
    s_paired = float(pr.shape[0] * nrow * nseq)
    dims = (nrow, ncol, nseq, chans, lengths.shape[0], ni, nj, nz, s_paired)
    half = nrow // 2
    tall = ni * chans
    vm = pl.BlockSpec(memory_space=pltpu.VMEM)
    hbm = pl.BlockSpec(memory_space=pltpu.HBM)
    sm = pl.BlockSpec(memory_space=pltpu.SMEM)
    dma = pltpu.SemaphoreType.DMA
    hj = nj // nseq
    return pl.pallas_call(
        functools.partial(kernel, dims),
        out_shape=jax.ShapeDtypeStruct((ni, hj, nz), BF16),
        in_specs=[hbm] * 5 + [vm] + [sm] * 2,
        out_specs=vm,
        scratch_shapes=[
            pltpu.VMEM(pr.shape, BF16),
            pltpu.VMEM(ur.shape, BF16),
            pltpu.VMEM((chans, ni, pl_.shape[0]), BF16),
            pltpu.VMEM((chans, ni, ul.shape[0]), BF16),
            pltpu.VMEM(weight.shape, BF16),
            pltpu.VMEM((tall, tall), BF16),
            pltpu.VMEM((nz, tall), BF16),
            pltpu.VMEM((nrow, pr.shape[0], chans * nj), BF16),
            pltpu.VMEM((nrow, ur.shape[0], chans * nj), BF16),
            pltpu.VMEM((ncol, pl_.shape[0], tall), BF16),
            pltpu.VMEM((tall, ncol * pl_.shape[0]), BF16),
            pltpu.VMEM((tall, ncol * ul.shape[0]), BF16),
            pltpu.VMEM((nz, ni * nj), F32),
            pltpu.VMEM((ni, nj, nz), F32),
            pltpu.VMEM((ni, hj, nz), F32),
            pltpu.VMEM((ni, nj), F32),
            pltpu.VMEM((ni, nj), F32),
            dma((2 * PHASES * half * 2,)),
            dma((2 * PHASES * half * 2,)),
            dma(((ncol - 1) * 2,)),
            dma(((ncol - 1) * 2,)),
            dma((ni // TAIL_UNIT,)),
            dma((ni // TAIL_UNIT,)),
            dma((5,)),
        ],
        compiler_params=pltpu.CompilerParams(
            collective_id=0, has_side_effects=True, vmem_limit_bytes=67043328 - 600 * 1024
        ),
    )(
        pr,
        ur,
        jnp.transpose(pl_, (1, 2, 0)),
        jnp.transpose(ul, (1, 2, 0)),
        weight,
        bias.reshape(1, nz),
        lengths,
        depths,
    )


def solution(mesh):
    sizes = (mesh.shape["row"], mesh.shape["col"], mesh.shape["seq"])
    return jax.shard_map(
        functools.partial(body, sizes),
        mesh=mesh,
        in_specs=(
            P(("groups", "seq", "col"), None, "row"),
            P(("groups", "seq", "row"), None, "col"),
            P(("groups", "seq", "col"), None, "row"),
            P(("groups", "seq", "row"), None, "col"),
            P(),
            P(),
            P("groups"),
            P("groups"),
        ),
        out_specs=P(("groups", "row"), ("col", "seq"), None),
        check_vma=False,
    )
```
